512 devices in a mesh: dp: 8 (over z), vocab: 64 (over x, y, core).
Axes of the slice: x: 4, y: 8, z: 8, core: 2. Of those that a mesh axis runs over, the one named last changes fastest.
Arguments:
- hidden: bfloat16 [384, 8192], P('dp', 'vocab'), may hold values from -90 to 90
- weight: bfloat16 [8192, 152064], P('dp', 'vocab'), may hold values from -0.1875 to 0.1875
- targets: int32 [384], P('dp'), may hold values from 0 to 152063
- pad_mask: int32 [384], P('dp'), may hold values from 0 to 1
Outputs:
- token_nll: float32 [384], P('dp')
- nll_total: float32 [], replicated
The draws below stay inside these ranges and needn't reach their ends.
All inputs are finite; a program needn't handle non-finite values.
Results may differ from the reference program's by a relative error of at most 0.0003.
Values may be sent and summed in bfloat16 or wider, within the bound.
A program may use at most 64 MiB of HBM per device.

```python
import math
import jax
import jax.numpy as jnp
import numpy as np

D = 8192
TOKENS = 384
VOCAB = 152064
N_DP = 8


def draw_hidden(key, part):
    base = jax.random.truncated_normal(key, -6.0, 6.0, (TOKENS, D), jnp.float32)
    return base.astype(jnp.bfloat16)


def draw_pad_mask(key, part):
    positions = jnp.arange(TOKENS)
    level = 25 + 70 * positions // TOKENS
    return (jax.random.randint(key, (TOKENS,), 0, 100) < level).astype(jnp.int32)


def touch_ends(values, own_key, least, largest):
    shape = values.shape
    place = [jax.random.randint(jax.random.fold_in(own_key, axis), (), 0, shape[axis]) for axis in range(len(shape))]
    values = values.at[tuple(place)].set(least)
    longest = shape.index(max(shape))
    place[longest] = (place[longest] + 1) % shape[longest]
    return values.at[tuple(place)].set(largest)


def levels(rng, dims, shards, low, high):
    factor_of, own = 1.0, jax.random.fold_in(rng, 6)
    for dim, shards_of in shards:
        heights = jnp.exp(jax.random.uniform(jax.random.fold_in(own, dim), (shards_of,), jnp.float32, low / len(shards), high / len(shards)))
        factor_of = factor_of * jnp.repeat(heights, dims[dim] // shards_of).reshape([-1 if axis == dim else 1 for axis in range(len(dims))])
    return factor_of


def wide_ids(stream_key, extent, count, skew):
    loads = [min(1 << octave, count + 1 - (1 << octave)) * (1 << 20) // math.isqrt((1 << octave) ** skew) + 1 for octave in range((count + 1).bit_length()) if 1 << octave <= count]
    scale = 1 + sum(loads) // (1 << 30)
    listing = np.cumsum(np.array([max(1, weight // scale) for weight in loads]))
    lot = jax.random.randint(jax.random.fold_in(stream_key, 1), extent, 0, int(listing[len(loads) - 1]))
    start = jnp.left_shift(1, jnp.searchsorted(jnp.asarray(listing, jnp.int32), lot, side="right").astype(jnp.int32))
    standing = start - 1 + jax.random.randint(jax.random.fold_in(stream_key, 4), extent, 0, 1 << 30) % jnp.minimum(start, count + 1 - start)
    return jax.random.permutation(jax.random.fold_in(stream_key, 2), count)[standing].astype(jnp.int32)


def noise(key, extent, deviation, limit, split=(), dtype=jnp.bfloat16):
    result = jax.random.normal(key, extent, jnp.float32) * deviation
    if len(split) > 0:
        result = levels(key, extent, split, -0.22, 0.18) * result
    return jnp.clip(result, min=-limit, max=limit).astype(dtype)


def setup_inputs(seed: int = 0) -> dict:
    keys = jax.random.split(jax.random.key(seed), 5)
    hidden = draw_hidden(jax.random.fold_in(keys[4], 71), 0)
    weight = noise(keys[1], (D, VOCAB), (D // 9) ** -0.5, 0.1875, ((0, 8), (1, 64)))
    targets = touch_ends(wide_ids(keys[2], (TOKENS,), VOCAB, 2), jax.random.fold_in(keys[2], 3), 0, VOCAB - 1).astype(jnp.int32)
    pad_mask = draw_pad_mask(jax.random.fold_in(keys[4], 71), 0)
    return {"hidden": hidden, "weight": weight, "targets": targets, "pad_mask": pad_mask}


def reference(hidden, weight, targets, pad_mask):
    slab = D // N_DP
    logits = jnp.zeros((TOKENS, VOCAB), jnp.float32)
    for block in range(N_DP):
        partial_value = jnp.dot(hidden[:, block * slab:(block + 1) * slab], weight[block * slab:(block + 1) * slab, :], preferred_element_type=jnp.float32)
        logits = logits + partial_value
    row_max = jnp.max(logits, axis=1)
    exp_sum = jnp.sum(jnp.exp(logits - row_max[:, None]), axis=1)
    picked = jnp.take_along_axis(logits, targets[:, None].astype(jnp.int32), axis=1)[:, 0]
    token_nll = pad_mask.astype(jnp.float32) * (row_max + jnp.log(exp_sum) - picked)
    return token_nll, jnp.sum(token_nll)
```

```python
import functools

import jax
import jax.numpy as jnp
from jax import lax
from jax.experimental import pallas as pl
from jax.experimental.pallas import tpu as pltpu
from jax.sharding import PartitionSpec as P

NZ, NX, NY, NC = 8, 4, 8, 2
T = 48
D = 128
CH = 16
NCH = T // CH
LN2 = 0.6931471805599453
TOP = 32766.0
F32 = jnp.float32


def kernel(V, VP, hid, weight, tgt, msk, nll_out, tot_out,
           H, W, ACC, SB, RB, TQ, MQ, MB1, MB2, MB3,
           w_sem, zs_sem, own_r, s1_s, s2_s, s3_s, s3_r, s4_s, s4_r,
           q_s, q_r, ring_s, ring_r, m_s, m_r):
    z = lax.axis_index("dp")
    v = lax.axis_index("vocab")
    c = lax.rem(v, NC)
    y = lax.rem(lax.div(v, NC), NY)
    x = lax.div(v, NC * NY)
    r = lax.rem(y, 4)
    xc = x * NC + c
    sg = 1 - 2 * c

    def at(zz=z, xx=x, yy=y, cc=c):
        return (zz, (xx * NY + yy) * NC + cc)

    def remote(src, dst, ss, rs, dev):
        return pltpu.make_async_remote_copy(
            src_ref=src, dst_ref=dst, send_sem=ss, recv_sem=rs,
            device_id=dev, device_id_type=pl.DeviceIdType.MESH)

    wcopies = []
    for cc in range(NC):
        for rr in range(4):
            wcopies.append(pltpu.make_async_copy(
                weight.at[pl.ds((rr * NC + cc) * D, D)],
                W.at[pl.ds((cc * 4 + rr) * D, D)], w_sem.at[cc * 4 + rr]))
    for cp in wcopies:
        cp.start()

    def xc_peer(d):
        o = lax.rem(xc + d, 8)
        return o, at(xx=lax.div(o, NC), cc=lax.rem(o, NC))

    def y_peer(d):
        o = lax.rem(y + d, NY)
        return o, at(yy=o)

    def z_peer(d):
        o = lax.rem(z + d, NZ)
        return o, at(zz=o)

    peers = (xc_peer, y_peer, z_peer)
    barrier = pltpu.get_barrier_semaphore()
    for peer in peers:
        for d in range(1, 8):
            pl.semaphore_signal(barrier, inc=1, device_id=peer(d)[1],
                                device_id_type=pl.DeviceIdType.MESH)
    pl.semaphore_wait(barrier, 21)

    def rows(o):
        return pl.ds(pl.multiple_of(o * T, CH), T)

    kd = 2 * x + lax.div(y, 4)
    zoff = lax.rem(z - kd + NZ, NZ)
    zmove = remote(hid, H.at[c, r, rows(zoff)], zs_sem, own_r.at[zoff], at(zz=kd))
    zlocal = pltpu.make_async_copy(hid, H.at[c, r, rows(zoff)], own_r.at[zoff])

    @pl.when(z != kd)
    def _():
        zmove.start()

    @pl.when(z == kd)
    def _():
        zlocal.start()

    opp = lax.rem(z + 4, NZ)
    tcopy = remote(tgt, TQ, q_s.at[0], q_r.at[0], at(zz=opp))
    mcopy = remote(msk, MQ, q_s.at[1], q_r.at[1], at(zz=opp))
    tcopy.start()
    mcopy.start()

    xs = lax.div(z, 2)
    in_col = x == xs
    is_src = jnp.logical_and(in_col, lax.div(y, 4) == lax.rem(z, 2))

    def s1(o):
        b = H.at[c, r, rows(o)]
        return remote(b, b, s1_s.at[o], own_r.at[o], at(yy=lax.rem(y + 4, NY)))

    def s2(o, d):
        b = H.at[c, r, rows(o)]
        return remote(b, b, s2_s.at[o, d - 1], own_r.at[o], at(xx=lax.rem(x + d, NX)))

    steps3 = (1, NY - 1, 2 * sg + NY)

    def s3(o, n):
        b = H.at[c, r, rows(o)]
        return remote(b, b, s3_s.at[o, n], s3_r.at[o, n], at(yy=lax.rem(y + steps3[n], NY)))

    def s4(o):
        b = H.at[c, :, rows(o)]
        return remote(b, b, s4_s.at[o], s4_r.at[o], at(cc=1 - c))

    def take_own(o):
        zlocal_o = pltpu.make_async_copy(hid, H.at[c, r, rows(o)], own_r.at[o])
        zlocal_o.wait()

        @pl.when(is_src)
        def _():
            s1(o).start()

        @pl.when(in_col)
        def _():
            for d in range(1, NX):
                s2(o, d).start()

        for n in range(3):
            s3(o, n).start()

    def take_y(o):
        for n in range(3):
            s3(o, n).wait_recv()
        s4(o).start()

    def take_core(o):
        s4(o).wait_recv()

    lane = lax.broadcasted_iota(jnp.int32, (CH, VP), 1)
    valid = lane < V

    def mm(n, o):
        o = lax.rem(o + NZ, NZ)
        rs = rows(o)
        lhs = jnp.concatenate([H[cc, rr, rs, :] for cc in range(NC) for rr in range(4)], axis=1)
        main = V // 256 * 256
        for a in range(0, main, 768):
            w = min(768, main - a)
            ACC[n, :, a:a + w] = jnp.dot(lhs, W[:, a:a + w], preferred_element_type=F32)
        if main < V:
            ACC[n, :, main:V] = jnp.dot(lhs, W[:, main:V], preferred_element_type=F32)

    def taken(n, k):
        q = RB[n, pl.ds(k * CH, CH), :].astype(F32)
        g = jnp.exp(q[:, VP - 1:VP] * (LN2 / 64)) * (1.0 / TOP)
        return q * g

    def ring(n, k, dz):
        b = pl.ds(k * CH, CH)
        return remote(SB.at[n, b], RB.at[n, b], ring_s.at[n, k], ring_r.at[n, k],
                      at(zz=lax.rem(z + dz + NZ, NZ)))

    def send(n, k, val, dz):
        top = jnp.max(jnp.where(valid, jnp.abs(val), 0.0), axis=1, keepdims=True)
        code = jnp.ceil(jnp.log(jnp.maximum(top, 1e-30)) * (64 / LN2)) + 1.0
        q = val * (jnp.exp(code * (-LN2 / 64)) * TOP)
        SB[n, pl.ds(k * CH, CH), :] = jnp.round(jnp.where(valid, q, code)).astype(jnp.int16)
        ring(n, k, dz).start()

    def first(n, dz):
        for k in range(NCH):
            send(n, k, ACC[n, pl.ds(k * CH, CH), :], dz)

    def onward(n, k, dz):
        ring(n - 1, k, dz).wait_recv()
        send(n, k, ACC[n, pl.ds(k * CH, CH), :] + taken(n - 1, k), dz)

    take_own(0)
    take_own(1)
    take_own(7)
    take_y(0)
    take_own(2)
    take_own(6)
    take_core(0)
    for cp in wcopies:
        cp.wait()
    mm(0, 0)
    first(0, sg)
    take_y(1)
    take_y(7)
    take_own(3)
    take_own(5)
    take_own(4)
    take_core(1)
    take_core(7)
    mm(4, sg)
    first(4, -sg)
    mm(1, -sg)
    take_y(2)
    take_y(6)
    take_y(3)
    take_y(5)
    take_y(4)
    take_core(2)
    take_core(6)
    mm(5, 2 * sg)
    for k in range(NCH):
        onward(1, k, sg)
        onward(5, k, -sg)
    take_core(3)
    take_core(5)
    take_core(4)
    mm(2, -2 * sg)
    mm(6, 3 * sg)
    for k in range(NCH):
        onward(2, k, sg)
        onward(6, k, -sg)
    mm(3, -3 * sg)
    mm(7, 4 * sg)
    for k in range(NCH):
        onward(3, k, sg)

    tcopy.wait_recv()
    mcopy.wait_recv()
    ri = lax.broadcasted_iota(jnp.int32, (T, T), 0)
    ci = lax.broadcasted_iota(jnp.int32, (T, T), 1)
    tcol = jnp.sum(jnp.where(ri == ci, TQ[...].astype(F32), 0.0), axis=1, keepdims=True).astype(jnp.int32)
    ids = jnp.where(valid, lane + v * V, -1)
    cols = []
    for k in range(NCH):
        b = pl.ds(k * CH, CH)
        ring(3, k, sg).wait_recv()
        ring(6, k, -sg).wait_recv()
        val = ACC[7, b, :] + taken(3, k) + taken(6, k)
        val = jnp.where(valid, val, -3e38)
        top = jnp.max(val, axis=1, keepdims=True)
        s = jnp.sum(jnp.exp(val - top), axis=1, keepdims=True)
        p = jnp.sum(jnp.where(ids == tcol[k * CH:(k + 1) * CH], val, 0.0), axis=1, keepdims=True)
        cols.append((top, s, p))

    rl = lax.broadcasted_iota(jnp.int32, (T, 128), 0)
    ll = lax.broadcasted_iota(jnp.int32, (T, 128), 1)

    def as_row(n):
        col = jnp.concatenate([t[n] for t in cols], axis=0)
        return jnp.sum(jnp.where(rl == ll, col, 0.0), axis=0, keepdims=True)

    def exchange(MB, me, peer, base, rws):
        for n, row in enumerate(rws):
            MB[me, n:n + 1, :] = row
        cps = []
        for d in range(1, 8):
            o, dev = peer(d)
            cps.append(remote(MB.at[me], MB.at[me], m_s.at[base, d], m_r.at[base, me], dev))
        for cp in cps:
            cp.start()
        for d in range(1, 8):
            o, dev = peer(d)
            remote(MB.at[o], MB.at[o], m_s.at[base, d], m_r.at[base, o], dev).wait_recv()
        return cps

    def merged(MB):
        ms = [MB[j, 0:1, :] for j in range(8)]
        top = functools.reduce(jnp.maximum, ms)
        s = sum(MB[j, 1:2, :] * jnp.exp(ms[j] - top) for j in range(8))
        p = sum(MB[j, 2:3, :] for j in range(8))
        return top, s, p

    left = exchange(MB1, xc, xc_peer, 0, (as_row(0), as_row(1), as_row(2)))
    left += exchange(MB2, y, y_peer, 1, merged(MB1))
    top, s, p = merged(MB2)
    inside = lax.broadcasted_iota(jnp.int32, (1, 128), 1) < T
    nll = jnp.where(inside, top + jnp.log(jnp.where(inside, s, 1.0)) - p, 0.0)[:, :T]
    nll = MQ[...].astype(F32) * nll
    total = jnp.sum(nll, axis=1, keepdims=True)
    nll128 = jnp.concatenate([nll, jnp.zeros((1, 128 - T), F32)], axis=1)
    left += exchange(MB3, z, z_peer, 2, (nll128, jnp.broadcast_to(total, (1, 128))))
    nll_out[...] = MB3[opp, 0:1, :][:, :T]
    tot_out[...] = sum(MB3[j, 1:2, :] for j in range(8))[:, 0:1]

    @pl.when(z != kd)
    def _():
        zmove.wait_send()

    tcopy.wait_send()
    mcopy.wait_send()
    for o in range(NZ):
        @pl.when(is_src)
        def _():
            s1(o).wait_send()

        @pl.when(in_col)
        def _():
            for d in range(1, NX):
                s2(o, d).wait_send()

        for n in range(3):
            s3(o, n).wait_send()
        s4(o).wait_send()
    for n in range(7):
        for k in range(NCH):
            ring(n, k, sg).wait_send()
    for cp in left:
        cp.wait_send()


def per_device(hidden, weight, targets, pad_mask):
    V = weight.shape[1]
    VP = -(-(V + 1) // 128) * 128
    K = weight.shape[0]
    vmem = pl.BlockSpec(memory_space=pltpu.VMEM)
    dma = pltpu.SemaphoreType.DMA
    nll, tot = pl.pallas_call(
        functools.partial(kernel, V, VP),
        out_shape=(jax.ShapeDtypeStruct((1, T), F32), jax.ShapeDtypeStruct((1, 1), F32)),
        in_specs=[vmem, pl.BlockSpec(memory_space=pl.ANY), vmem, vmem],
        out_specs=(vmem, vmem),
        scratch_shapes=[
            pltpu.VMEM((NC, 4, NZ * T, D), jnp.bfloat16),
            pltpu.VMEM((K, V), jnp.bfloat16),
            pltpu.VMEM((8, T, VP), F32),
            pltpu.VMEM((7, T, VP), jnp.int16),
            pltpu.VMEM((7, T, VP), jnp.int16),
            pltpu.VMEM((1, T), jnp.int32),
            pltpu.VMEM((1, T), jnp.int32),
            pltpu.VMEM((8, 8, 128), F32),
            pltpu.VMEM((8, 8, 128), F32),
            pltpu.VMEM((8, 8, 128), F32),
            dma((8,)), dma, dma((8,)), dma((8,)), dma((8, 3)), dma((8, 3)), dma((8, 3)),
            dma((8,)), dma((8,)), dma((2,)), dma((2,)), dma((7, NCH)), dma((7, NCH)),
            dma((3, 8)), dma((3, 8)),
        ],
        compiler_params=pltpu.CompilerParams(collective_id=0, has_side_effects=True),
    )(hidden, weight, targets.reshape(1, T), pad_mask.reshape(1, T))
    return nll.reshape(T), tot.reshape(())


def solution(mesh):
    placed = (P("dp", "vocab"), P("dp", "vocab"), P("dp"), P("dp"))
    return jax.shard_map(
        per_device, mesh=mesh, in_specs=placed, out_specs=(P("dp"), P()), check_vma=False
    )
```

```python
import functools

import jax
import jax.numpy as jnp
from jax import lax
from jax.experimental import pallas as pl
from jax.experimental.pallas import tpu as pltpu
from jax.sharding import PartitionSpec as P

NZ, NX, NY, NC = 8, 4, 8, 2
NV = NX * NY * NC
T = 48
D = 128
CH = 16
NCH = T // CH
HALF = 64
LN2 = 0.6931471805599453
TOP = 32766.0
F32 = jnp.float32
scope = jax.named_scope


def kernel(V, VP, hid, weight, tgt, msk, out,
           L, H, W, ACC, SB, RB, TM, ST, MB3,
           in_sem, zs_sem, src_r, own_r, s1_s, s2_s, s2_r,
           q_s, q_r, ring_s, ring_r, st_s, st_r, m_s, m_r, met):
    z = lax.axis_index("dp")
    v = lax.axis_index("vocab")
    c = lax.rem(v, NC)
    y = lax.rem(lax.div(v, NC), NY)
    x = lax.div(v, NC * NY)
    px, py = lax.rem(x, 2), lax.rem(y, 2)
    me = c * 4 + 2 * px + py
    sg = 1 - 2 * c

    def at(dz=0, dx=0, dy=0, dc=0):
        return (lax.rem(z + dz + NZ, NZ),
                (lax.rem(x + dx, NX) * NY + lax.rem(y + dy + NY, NY)) * NC + lax.rem(c + dc, NC))

    def remote(src, dst, ss, rs, dev):
        return pltpu.make_async_remote_copy(
            src_ref=src, dst_ref=dst, send_sem=ss, recv_sem=rs,
            device_id=dev, device_id_type=pl.DeviceIdType.MESH)

    def arrived(ref, sem):
        pltpu.make_async_copy(ref, ref, sem).wait()

    def signal(sem, dev):
        pl.semaphore_signal(sem, inc=1, device_id=dev, device_id_type=pl.DeviceIdType.MESH)

    near = [(dx, dy, dc) for dx, dy in ((1, 1), (3, -1), (1, 0), (3, 0), (0, 1), (0, -1)) for dc in (0, 1)] + [(0, 0, 1)]
    far = [(dx, dy, 0) for dy in (4, 2, -2, 0) for dx in (2, 1, 3, 0)]
    far = [d for d in far if d != (0, 0, 0) and d not in near]
    barrier = pltpu.get_barrier_semaphore()
    with scope("barrier"):
        for dx, dy, dc in far:
            signal(barrier, at(dx=dx, dy=dy, dc=dc))
        for dz in (4, 3, 5, 2, 6, 1, 7):
            signal(barrier, at(dz=dz))
        for dx, dy, dc in near:
            signal(barrier, at(dx=dx, dy=dy, dc=dc))

        wcopy = pltpu.make_async_copy(weight, W, in_sem)
        wcopy.start()
        pl.semaphore_wait(barrier, len(far) + 7 + len(near))

    def rows(o):
        return pl.ds(pl.multiple_of(o * T, CH), T)

    kd = 2 * x + lax.div(y, 4)
    zoff = lax.rem(z - kd + NZ, NZ)
    zmove = remote(hid, L.at[rows(zoff)], zs_sem, src_r.at[zoff], (kd, v))
    zlocal = pltpu.make_async_copy(hid, L.at[rows(0)], src_r.at[0])

    @pl.when(z != kd)
    def _():
        zmove.start()

    @pl.when(z == kd)
    def _():
        zlocal.start()

    tcopy = remote(tgt, TM.at[0], q_s, q_r, at(dz=4))
    mcopy = remote(msk, TM.at[1], q_s, q_r, at(dz=4))
    tcopy.start()
    mcopy.start()
    for dy, dc in ((-1, 0), (-1, 1), (0, 1)):
        signal(met, at(dy=dy, dc=dc))

    is_src = jnp.logical_and(x == lax.div(z, 2), lax.div(y, 4) == lax.rem(z, 2))

    q = lax.rem(y, 4)
    odd = lax.rem(lax.div(q, 2) + x, 2)
    spread = [(dx, dy) for dy in (4, 2, -2, 0) for dx in (2, 0)]
    mine = c * 4 + q

    def s1(o, n):
        dx, dy = spread[n]
        return remote(L.at[rows(o)], H.at[mine, rows(o)], s1_s, own_r.at[o], at(dx=dx + odd, dy=dy))

    def s1_here(o):
        return pltpu.make_async_copy(L.at[rows(o)], H.at[mine, rows(o)], own_r.at[o])

    fx, fy = sg + NX, sg
    hops = [(fx, fy, 1), (fx, fy, 0), (fx, 0, 1), (0, fy, 1), (fx, 0, 0), (0, fy, 0), (0, 0, 1)]

    def s2(o, n):
        b = H.at[me, rows(o)]
        return remote(b, b, s2_s, s2_r.at[o], at(dx=hops[n][0], dy=hops[n][1], dc=hops[n][2]))

    def from_source(*offs):
        with scope(f"src{offs[0]}"):
            @pl.when(is_src)
            def _():
                for o in offs:
                    arrived(L.at[rows(o)], src_r.at[o])
                    for n in range(7):
                        s1(o, n).start()

                    @pl.when(odd == 1)
                    def _():
                        s1(o, 7).start()

                    @pl.when(odd == 0)
                    def _():
                        s1_here(o).start()

    def take_own(*offs):
        with scope(f"own{offs[0]}"):
            for o in offs:
                arrived(H.at[me, rows(o)], own_r.at[o])
                for n in range(len(hops)):
                    s2(o, n).start()

    def take_all(*offs):
        with scope(f"all{offs[0]}"):
            for o in offs:
                arrived(H.at[0, 0:len(hops) * T], s2_r.at[o])

    lane = lax.broadcasted_iota(jnp.int32, (CH, VP), 1)
    valid = lane < V

    def mm(*offs):
        with scope(f"mm{offs[0]}"):
            lhs = jnp.concatenate([
                jnp.concatenate([H[cc * 4 + rr, rows(o), :] for rr in range(4) for cc in range(NC)], axis=1)
                for o in offs], axis=0)
            main = V // 256 * 256
            for a in [*range(0, main, 768), main]:
                w = min(768, main - a) or V - a
                if w:
                    res = lax.dot_general(lhs, W[a:a + w, :], (((1,), (1,)), ((), ())),
                                          preferred_element_type=F32)
                    for n, o in enumerate(offs):
                        ACC[o, :, a:a + w] = res[n * T:(n + 1) * T]

    def part(o, k):
        return ACC[lax.rem(o + NZ, NZ), pl.ds(k * CH, CH), :]

    def taken(n, k):
        q = RB[n, pl.ds(k * CH, CH), :].astype(F32)
        g = jnp.exp(q[:, VP - 1:VP] * (LN2 / 64)) * (1.0 / TOP)
        return q * g

    def ring(n, k):
        b = pl.ds(k * CH, CH)
        return remote(SB.at[n, b], RB.at[n, b], ring_s, ring_r.at[n, k],
                      at(dz=sg if n < 4 else -sg))

    def send(n, k, val):
        top = jnp.max(jnp.where(valid, jnp.abs(val), 0.0), axis=1, keepdims=True)
        code = jnp.ceil(jnp.log(jnp.maximum(top, 1e-30)) * (64 / LN2)) + 1.0
        q = val * (jnp.exp(code * (-LN2 / 64)) * TOP)
        SB[n, pl.ds(k * CH, CH), :] = jnp.round(jnp.where(valid, q, code)).astype(jnp.int16)
        ring(n, k).start()

    def block_of(n):
        return -n * sg if n < 4 else (n - 3) * sg

    def first(n):
        with scope(f"first{n}"):
            for k in range(NCH):
                send(n, k, part(block_of(n), k))

    def onward(n, k):
        with scope(f"ring{n}"):
            ring(n - 1, k).wait_recv()
            send(n, k, part(block_of(n), k) + taken(n - 1, k))

    from_source(0)
    take_own(0)
    from_source(1, 7, 2, 6)
    take_all(0)
    take_own(1, 7)
    take_own(2, 6)
    with scope("wwait"):
        wcopy.wait()
    mm(0)
    first(0)
    from_source(3, 5, 4)
    take_all(1, 7)
    mm(1, 7)
    first(4)
    for k in range(NCH):
        onward(1, k)
    take_own(3, 5, 4)
    take_all(2, 6)
    mm(2, 6)
    for k in range(NCH):
        onward(5, k)
        onward(2, k)
    take_all(3, 5, 4)
    mm(3, 5, 4)
    for k in range(NCH):
        onward(6, k)
        onward(3, k)

    arrived(TM, q_r)
    ri = lax.broadcasted_iota(jnp.int32, (T, T), 0)
    ci = lax.broadcasted_iota(jnp.int32, (T, T), 1)
    tcol = jnp.sum(jnp.where(ri == ci, TM[0].astype(F32), 0.0), axis=1, keepdims=True).astype(jnp.int32)
    ids = jnp.where(valid, lane + v * V, -1)
    lses, picks = [], []
    for k in range(NCH):
        with scope("last"):
            ring(3, k).wait_recv()
            ring(6, k).wait_recv()
        val = part(4, k) + taken(3, k) + taken(6, k)
        val = jnp.where(valid, val, -3e38)
        top = jnp.max(val, axis=1, keepdims=True)
        s = jnp.sum(jnp.exp(val - top), axis=1, keepdims=True)
        picks.append(jnp.sum(jnp.where(ids == tcol[k * CH:(k + 1) * CH], val, 0.0), axis=1, keepdims=True))
        lses.append(top + jnp.log(s))

    rl = lax.broadcasted_iota(jnp.int32, (T, 128), 0)
    ll = lax.broadcasted_iota(jnp.int32, (T, 128), 1)
    both = jnp.where(rl == ll, jnp.concatenate(lses, axis=0),
                     jnp.where(rl + HALF == ll, jnp.concatenate(picks, axis=0), 0.0))
    with scope("plane"):
        pl.semaphore_wait(met, 3)
        ST[v] = jnp.sum(both, axis=0, keepdims=True)

        def stat(d):
            o = lax.rem(v + d, NV)
            return remote(ST.at[v], ST.at[v], st_s, st_r, (z, o))

        for d in range(1, NV):
            stat(d).start()
        arrived(ST.at[0:NV - 1], st_r)
        st = ST[...].reshape(NV, 128)
        top = jnp.max(st, axis=0, keepdims=True)
        lse = top + jnp.log(jnp.sum(jnp.exp(st - top), axis=0, keepdims=True))
        picked = jnp.sum(st, axis=0, keepdims=True)
        nll = TM[1].astype(F32) * (lse[:, :T] - picked[:, HALF:HALF + T])
        total = jnp.sum(nll, axis=1, keepdims=True)

    with scope("zmerge"):
        MB3[z, :, 0:T] = nll
        MB3[z, :, HALF:128] = jnp.broadcast_to(total, (1, 128 - HALF))

        def across(d):
            return remote(MB3.at[z], MB3.at[z], m_s, m_r, at(dz=d))

        for d in (4, 3, 5, 2, 6, 1, 7):
            across(d).start()
        arrived(MB3.at[0:NZ - 1], m_r)
        opp = lax.rem(z + 4, NZ)
        out[:, 0:HALF] = MB3[opp, :, 0:HALF]
        out[:, HALF:128] = sum(MB3[j, :, HALF:128] for j in range(NZ))

    with scope("drain"):
        @pl.when(z != kd)
        def _():
            zmove.wait_send()

        arrived(TM, q_s)

        @pl.when(is_src)
        def _():
            arrived(H.at[0:7], s1_s)

            @pl.when(odd == 1)
            def _():
                arrived(H.at[0], s1_s)

        arrived(H.at[0:len(hops)], s2_s)
        arrived(SB, ring_s)
        arrived(ST.at[0:NV - 1], st_s)
        arrived(MB3.at[0:NZ - 1], m_s)


def per_device(hidden, weight, targets, pad_mask):
    K, V = weight.shape
    VP = -(-(V + 1) // 128) * 128
    hbm = pl.BlockSpec(memory_space=pl.ANY)
    dma = pltpu.SemaphoreType.DMA
    out = pl.pallas_call(
        functools.partial(kernel, V, VP),
        out_shape=jax.ShapeDtypeStruct((1, 128), F32),
        in_specs=[hbm] * 4,
        out_specs=pl.BlockSpec(memory_space=pltpu.VMEM),
        scratch_shapes=[
            pltpu.VMEM((NZ * T, D), jnp.bfloat16),
            pltpu.VMEM((NC * 4, NZ * T, D), jnp.bfloat16),
            pltpu.VMEM((V, K), jnp.bfloat16),
            pltpu.VMEM((8, T, VP), F32),
            pltpu.VMEM((7, T, VP), jnp.int16),
            pltpu.VMEM((7, T, VP), jnp.int16),
            pltpu.VMEM((2, 1, T), jnp.int32),
            pltpu.VMEM((NV, 1, 128), F32),
            pltpu.VMEM((NZ, 1, 128), F32),
            dma, dma, dma((8,)), dma((8,)), dma, dma, dma((8,)),
            dma, dma, dma, dma((7, NCH)), dma, dma, dma, dma,
            pltpu.SemaphoreType.REGULAR,
        ],
        compiler_params=pltpu.CompilerParams(collective_id=0, has_side_effects=True),
    )(hidden, weight.T, targets.reshape(1, T), pad_mask.reshape(1, T))
    return out[0, :T], out[0, HALF]


def solution(mesh):
    placed = (P("dp", "vocab"), P("dp", "vocab"), P("dp"), P("dp"))
    return jax.shard_map(
        per_device, mesh=mesh, in_specs=placed, out_specs=(P("dp"), P()), check_vma=False
    )
```
